32 devices in a mesh: grp: 8 (over y, x, core), sub: 4 (over z).
Axes of the slice: x: 2, y: 2, z: 4, core: 2. Of those that a mesh axis runs over, the one named last changes fastest.
Arguments:
- master: float32 [4096, 3584], P(('grp', 'sub')), may hold values from -120 to 120
- moment_one: float32 [4096, 3584], P(('grp', 'sub')), may hold values from -6 to 6
- moment_two: float32 [4096, 3584], P(('grp', 'sub')), may hold values from 0.01 to 4
- gradient: float32 [4096, 3584], P(('grp', 'sub')), may hold values from -120 to 120
- partner: int32 [32], replicated, may hold values from 0 to 31, each once
- tensor_of_row: int32 [4096], replicated, may hold values from 0 to 7, never falling along the last dimension, each value on 1 to 1024 neighbouring positions
Outputs:
- new_master: float32 [4096, 3584], P(('grp', 'sub'))
- new_moment_one: float32 [4096, 3584], P(('grp', 'sub'))
- new_moment_two: float32 [4096, 3584], P(('grp', 'sub'))
The draws below stay inside these ranges and needn't reach their ends.
Inputs may be any that keep to these rules, and one draw needn't show every extreme that they name: partner[n] is the device of new rank n; every device holds exactly one rank. `tensor_of_row`: tensor numbers never fall along the rows; each of the 8 tensors has one or more rows.
All inputs are finite; a program needn't handle non-finite values.
Results may differ from the reference program's by a relative error of at most 0.00007.
Values sent between devices are 32-bit elements; how exact they have to be, the bound alone decides.
A program may use at most 128 MiB of HBM per device.

```python
import math
import jax
import jax.numpy as jnp
import numpy as np
from jax import lax

W = 3584
ROWS_DEV = 128
LAYERS = 8
NDEV = 32
ROWS = 4096
BLOCK = 4


def scale_field(key, trend_pos):
    key_row, key_col = jax.random.split(key, 2)
    row_scale = jnp.exp(jax.random.uniform(key_row, (ROWS, 1), jnp.float32, 0.0, math.log(10.0)))
    col_scale = jnp.exp(jax.random.uniform(key_col, (1, W), jnp.float32, 0.0, math.log(10.0)))
    trend = jnp.power(3.0, trend_pos.astype(jnp.float32) / max(NDEV - 1, 1))
    return row_scale * col_scale * trend[:, None] / 15.0


def draw_master(key, part):
    key = jax.random.fold_in(key, 11)
    key_scale, key_noise = jax.random.split(key, 2)
    row_index = jnp.arange(ROWS, dtype=jnp.int32)
    trend_pos = row_index % ROWS_DEV // BLOCK
    noise = jax.random.normal(key_noise, (ROWS, W), jnp.float32)
    noise = jnp.clip(noise, -6.0, 6.0)
    return noise * scale_field(key_scale, trend_pos)


def draw_gradient(key, part):
    key = jax.random.fold_in(key, 23)
    key_scale, key_noise = jax.random.split(key, 2)
    row_index = jnp.arange(ROWS, dtype=jnp.int32)
    trend_pos = row_index // ROWS_DEV
    noise = jax.random.normal(key_noise, (ROWS, W), jnp.float32)
    noise = jnp.clip(noise, -6.0, 6.0)
    return noise * scale_field(key_scale, trend_pos)


def steps_of(rng, dims, pieces, smallest, top_value):
    gain, own = 1.0, jax.random.fold_in(rng, 6)
    for dim, shards_of in pieces:
        steps = jnp.exp(jax.random.uniform(jax.random.fold_in(own, dim), (shards_of,), jnp.float32, smallest / len(pieces), top_value / len(pieces)))
        gain = gain * jnp.repeat(steps, dims[dim] // shards_of).reshape([-1 if axis == dim else 1 for axis in range(len(dims))])
    return gain


def profile(count, total, bound, slope):
    loads = [(1 << 20) // math.isqrt(standing ** slope) + 1 for standing in range(2, count + 1)]
    surplus, given = total - bound - (count - 1), [1] * (count - 1)
    while surplus > 0:
        candidates = [i for i in range(count - 1) if given[i] < bound]
        pool, remaining = sum([loads[i] for i in candidates]), surplus
        for i in candidates:
            extra = min(bound - given[i], max(1, remaining * loads[i] // pool), surplus)
            given[i] = given[i] + extra
            surplus = surplus - extra
    return np.array([bound] + given)


def ragged_sizes(rng, number_of, total, bound, slope):
    if number_of == 2:
        one = jax.random.randint(rng, (), max(1, total - bound), min(bound, total - 1) + 1)
        return jnp.stack([one, total - one])
    sizes = jnp.asarray(profile(number_of, total, bound, slope), jnp.int32)
    twos = (number_of - 1) // 2
    donor, sink = sizes[1:1 + 2 * twos:2], sizes[2:2 + 2 * twos:2]
    slack = jnp.minimum(donor - 1, bound - sink)
    shifted = jax.random.randint(jax.random.fold_in(rng, 1), (twos,), 0, 1 << 20) % (slack + 1)
    sizes = sizes.at[1:1 + 2 * twos:2].set(donor - shifted).at[2:2 + 2 * twos:2].set(sink + shifted)
    return sizes[jax.random.permutation(jax.random.fold_in(rng, 2), number_of)]


def gaussian(own_key, extent, spread, bound, cuts=(), kind=jnp.bfloat16):
    entries = jax.random.normal(own_key, extent, jnp.float32) * spread
    if len(cuts) > 0:
        entries = steps_of(own_key, extent, cuts, -0.22, 0.18) * entries
    return jnp.clip(entries, min=-bound, max=bound).astype(kind)


def setup_inputs(seed: int = 0) -> dict:
    keys = jax.random.split(jax.random.key(seed), 7)
    return {
        "master": draw_master(jax.random.fold_in(keys[6], 71), 0),
        "moment_one": gaussian(keys[1], (ROWS, W), 1.0, 6.0, ((0, 32),), jnp.float32),
        "moment_two": jnp.clip(jnp.exp(math.log(4.0) - 5.9914646 * jax.random.uniform(keys[2], (ROWS, W), jnp.float32) ** steps_of(keys[2], (ROWS, W), ((0, 32),), -0.2, 0.2)), 0.01, 4.0),
        "gradient": draw_gradient(jax.random.fold_in(keys[6], 71), 0),
        "partner": jax.random.permutation(keys[4], NDEV).astype(jnp.int32),
        "tensor_of_row": jnp.searchsorted(jnp.cumsum(ragged_sizes(keys[5], LAYERS, ROWS, 2 * ROWS // LAYERS, 1)), jnp.arange(ROWS), side="right").astype(jnp.int32),
    }


beta_one = 0.9
beta_two = 0.999
step_count = 10
adam_eps = 1e-06
trust_eps = 1e-06
learn_rate = 0.05
decay_rate = 0.01

def reference(master, moment_one, moment_two, gradient, partner, tensor_of_row):
    total_rows = master.shape[0]
    row_index = jnp.arange(total_rows, dtype=jnp.int32)
    owner = row_index // ROWS_DEV
    inside = row_index % ROWS_DEV
    rank = inside // BLOCK
    offset = inside % BLOCK
    place = (partner[rank] * ROWS_DEV + owner * BLOCK + offset).astype(jnp.int32)
    grad_rows = gradient[place]
    first = beta_one * moment_one + (1.0 - beta_one) * grad_rows
    second = beta_two * moment_two + (1.0 - beta_two) * grad_rows * grad_rows
    correct_one = 1.0 - beta_one ** step_count
    correct_two = 1.0 - beta_two ** step_count
    update = first / correct_one / (jnp.sqrt(second / correct_two) + adam_eps) + decay_rate * master
    weight_sq = jax.ops.segment_sum(lax.optimization_barrier(jnp.sum(master * master, axis=1)), tensor_of_row, num_segments=LAYERS)
    update_sq = jax.ops.segment_sum(lax.optimization_barrier(jnp.sum(update * update, axis=1)), tensor_of_row, num_segments=LAYERS)
    ratio = jnp.sqrt(weight_sq) / (jnp.sqrt(update_sq) + trust_eps)
    row_ratio = ratio[tensor_of_row]
    fresh = master - learn_rate * row_ratio[:, None] * update

    def settle(values):
        return jnp.zeros_like(values).at[place].set(values)
    return (settle(fresh), settle(first), settle(second))
```

```python
import functools

import jax
import jax.numpy as jnp
from jax import lax
from jax.experimental import pallas as pl
from jax.experimental.pallas import tpu as pltpu
from jax.sharding import PartitionSpec as P

LAYERS = 8
LANES = 128
TILE = 8
MESH = pl.DeviceIdType.MESH

beta_one = 0.9
beta_two = 0.999
step_count = 10
adam_eps = 1e-06
trust_eps = 1e-06
learn_rate = 0.05
decay_rate = 0.01


def xor(a, b, bound):
    total, bit = 0, 1
    while bit < bound:
        total = total + ((a // bit + b // bit) % 2) * bit
        bit *= 2
    return total


def prepare(groups, subs, partner, ids, master_hbm, one_hbm, two_hbm, staged, row_ids,
            master, one, two, load_sem):
    devices = groups * subs
    rows_dev, width = master.shape
    block = rows_dev // devices
    many = TILE // block
    me = lax.axis_index("grp") * subs + lax.axis_index("sub")
    loads = [
        pltpu.make_async_copy(src, dst, load_sem.at[i])
        for i, (src, dst) in enumerate([(master_hbm, master), (one_hbm, one), (two_hbm, two)])
    ]
    for load in loads:
        load.start()

    def rank_of(device):
        def seek(n, found):
            return found + jnp.where(partner[n] == device, n, 0)

        return lax.fori_loop(0, devices, seek, jnp.int32(0), unroll=8)

    my_rank = rank_of(me)
    sub_iota = lax.broadcasted_iota(jnp.int32, (TILE, LANES), 0)

    def name_rows(s, carry):
        here = jnp.zeros((TILE, LANES), jnp.int32)
        for i in range(many):
            for b in range(block):
                tensor = ids[(s * many + i) * rows_dev + my_rank * block + b]
                here = jnp.where(sub_iota == i * block + b, tensor, here)
        row_ids[pl.ds(pl.multiple_of(s * TILE, TILE), TILE), :] = here
        return carry

    lax.fori_loop(0, rows_dev // TILE, name_rows, 0)
    for load in loads:
        load.wait()

    def stage(n, carry):
        peer = partner[n]
        base = pl.multiple_of((n // many) * TILE, TILE)
        part = n % many
        for a, source in enumerate((master, one, two)):
            rows = source[pl.ds(base, TILE), :]
            piece = rows[:block]
            for i in range(1, many):
                piece = jnp.where(part == i, rows[i * block : (i + 1) * block], piece)
            staged[peer, a] = piece
        return carry

    lax.fori_loop(0, devices, stage, 0)


def kernel(groups, subs, staged, row_ids, grad_hbm,
           fresh, first_out, second_out,
           grad, landed, update, acc_w, acc_u, sums,
           load_sem, send_sem, recv_sem, sum_send, sum_recv):
    devices = groups * subs
    rows_dev, width = grad.shape
    block = rows_dev // devices
    many = TILE // block
    tiles = rows_dev // TILE
    columns = width // LANES
    me = lax.axis_index("grp") * subs + lax.axis_index("sub")

    def at(peer):
        return {"grp": peer // subs, "sub": peer % subs}

    load = pltpu.make_async_copy(grad_hbm, grad, load_sem)
    load.start()
    barrier = pltpu.get_barrier_semaphore()

    def greet(k, carry):
        pl.semaphore_signal(barrier, inc=1, device_id=at(xor(me, k, devices)), device_id_type=MESH)
        return carry

    lax.fori_loop(1, devices, greet, 0)
    pl.semaphore_wait(barrier, devices - 1)

    def tile_at(s):
        halves = subs // many
        return (groups - 1 - s % groups) * halves + (halves - 1 - s // groups)

    def peer_at(t):
        return tile_at(t // many) * many + (many - 1 - t % many)

    def exchange(k):
        return pltpu.make_async_remote_copy(
            src_ref=staged.at[xor(me, k, devices)],
            dst_ref=landed.at[k],
            send_sem=send_sem.at[k],
            recv_sem=recv_sem.at[k],
            device_id=at(xor(me, k, devices)),
            device_id_type=MESH,
        )

    def send(t, carry):
        exchange(peer_at(t)).start()
        return carry

    lax.fori_loop(0, devices - 1, send, 0)
    landed[0] = staged[me]
    load.wait()
    acc_w[...] = jnp.zeros_like(acc_w)
    acc_u[...] = jnp.zeros_like(acc_u)
    sub_iota = lax.broadcasted_iota(jnp.int32, (TILE, LANES), 0)
    lane_iota = lax.broadcasted_iota(jnp.int32, (TILE, LANES), 1)
    scale_one = 1.0 / (1.0 - beta_one**step_count)
    scale_two = 1.0 / (1.0 - beta_two**step_count)

    def consume(j):
        first_owner = xor(me // many, j, devices // many) * many
        base = pl.multiple_of(first_owner * block, TILE)
        slots = [j * many + xor(me % many, i, many) for i in range(many)]
        here = row_ids[pl.ds(base, TILE), :]
        sum_w = jnp.zeros((TILE, LANES), jnp.float32)
        sum_u = jnp.zeros((TILE, LANES), jnp.float32)
        for c in range(columns):
            cut = slice(c * LANES, (c + 1) * LANES)

            def arrived(a):
                return jnp.concatenate([landed[slot, a, :, cut] for slot in slots], axis=0)

            g = grad[pl.ds(base, TILE), cut]
            w = arrived(0)
            first = beta_one * arrived(1) + (1.0 - beta_one) * g
            second = beta_two * arrived(2) + (1.0 - beta_two) * g * g
            u = (first * scale_one) / (jnp.sqrt(second * scale_two) + adam_eps) + decay_rate * w
            first_out[pl.ds(base, TILE), cut] = first
            second_out[pl.ds(base, TILE), cut] = second
            fresh[pl.ds(base, TILE), cut] = w
            update[pl.ds(base, TILE), cut] = u
            sum_w += w * w
            sum_u += u * u
        for t in range(LAYERS):
            acc_w[t] += jnp.where(here == t, sum_w, 0.0)
            acc_u[t] += jnp.where(here == t, sum_u, 0.0)

    def receive(s, carry):
        j = tile_at(s)
        for i in range(many):
            exchange(j * many + i).wait_recv()
        consume(j)
        return carry

    lax.fori_loop(0, tiles - 1, receive, 0)
    for i in range(1, many):
        exchange(i).wait_recv()
    consume(0)

    col_w = jnp.sum(jnp.sum(acc_w[...], axis=1), axis=1, keepdims=True)
    col_u = jnp.sum(jnp.sum(acc_u[...], axis=1), axis=1, keepdims=True)
    spread = jnp.where(lane_iota == sub_iota, col_w, 0.0) + jnp.where(
        lane_iota == sub_iota + LAYERS, col_u, 0.0
    )
    sums[0] = jnp.sum(spread, axis=0, keepdims=True)

    def exchange_sum(k):
        return pltpu.make_async_remote_copy(
            src_ref=sums.at[0],
            dst_ref=sums.at[k],
            send_sem=sum_send.at[k],
            recv_sem=sum_recv.at[k],
            device_id=at(xor(me, k, devices)),
            device_id_type=MESH,
        )

    def send_sum(t, carry):
        exchange_sum(devices - 1 - t).start()
        return carry

    lax.fori_loop(0, devices - 1, send_sum, 0)

    def drain(k, carry):
        exchange(k).wait_send()
        return carry

    lax.fori_loop(1, devices, drain, 0)

    def drain_sum(k, carry):
        exchange_sum(k).wait_recv()
        exchange_sum(k).wait_send()
        return carry

    lax.fori_loop(1, devices, drain_sum, 0)

    def gather_sum(o, total):
        return total + sums[xor(me, o, devices)]

    total = lax.fori_loop(0, devices, gather_sum, jnp.zeros((1, LANES), jnp.float32), unroll=8)
    wide = jnp.broadcast_to(total, (TILE, LANES))
    weight_sq = jnp.sum(jnp.where(lane_iota == sub_iota, wide, 0.0), axis=1, keepdims=True)
    update_sq = jnp.sum(jnp.where(lane_iota == sub_iota + LAYERS, wide, 0.0), axis=1, keepdims=True)
    ratio = learn_rate * (jnp.sqrt(weight_sq) / (jnp.sqrt(update_sq) + trust_eps))
    ratio = jnp.broadcast_to(ratio, (TILE, LANES))

    def finish(s, carry):
        base = pl.multiple_of(s * TILE, TILE)
        here = row_ids[pl.ds(base, TILE), :]
        step = jnp.zeros((TILE, LANES), jnp.float32)
        for t in range(LAYERS):
            step = jnp.where(here == t, jnp.broadcast_to(ratio[t : t + 1], (TILE, LANES)), step)
        for c in range(columns):
            cut = slice(c * LANES, (c + 1) * LANES)
            fresh[pl.ds(base, TILE), cut] -= step * update[pl.ds(base, TILE), cut]
        return carry

    lax.fori_loop(0, tiles, finish, 0)


def local(groups, subs, master, moment_one, moment_two, gradient, partner, tensor_of_row):
    rows_dev, width = master.shape
    devices = groups * subs
    block = rows_dev // devices
    whole = jax.ShapeDtypeStruct((rows_dev, width), jnp.float32)
    vmem = pl.BlockSpec(memory_space=pltpu.VMEM)
    smem = pl.BlockSpec(memory_space=pltpu.SMEM)
    hbm = pl.BlockSpec(memory_space=pl.ANY)
    slots = (devices, 3, block, width)
    staged, row_ids = pl.pallas_call(
        functools.partial(prepare, groups, subs),
        out_shape=(
            jax.ShapeDtypeStruct(slots, jnp.float32),
            jax.ShapeDtypeStruct((rows_dev, LANES), jnp.int32),
        ),
        in_specs=[smem, smem, hbm, hbm, hbm],
        out_specs=(vmem, vmem),
        scratch_shapes=[pltpu.VMEM((rows_dev, width), jnp.float32)] * 3
        + [pltpu.SemaphoreType.DMA((3,))],
        compiler_params=pltpu.CompilerParams(vmem_limit_bytes=32 * 1024 * 1024),
    )(partner, tensor_of_row, master, moment_one, moment_two)
    return pl.pallas_call(
        functools.partial(kernel, groups, subs),
        out_shape=(whole, whole, whole),
        in_specs=[vmem, vmem, hbm],
        out_specs=(vmem, vmem, vmem),
        scratch_shapes=[
            pltpu.VMEM((rows_dev, width), jnp.float32),
            pltpu.VMEM(slots, jnp.float32),
            pltpu.VMEM((rows_dev, width), jnp.float32),
            pltpu.VMEM((LAYERS, TILE, LANES), jnp.float32),
            pltpu.VMEM((LAYERS, TILE, LANES), jnp.float32),
            pltpu.VMEM((devices, 1, LANES), jnp.float32),
            pltpu.SemaphoreType.DMA,
            pltpu.SemaphoreType.DMA((devices,)),
            pltpu.SemaphoreType.DMA((devices,)),
            pltpu.SemaphoreType.DMA((devices,)),
            pltpu.SemaphoreType.DMA((devices,)),
        ],
        compiler_params=pltpu.CompilerParams(
            collective_id=0, has_side_effects=True, vmem_limit_bytes=40 * 1024 * 1024
        ),
    )(staged, row_ids, gradient)


def solution(mesh):
    rows = P(("grp", "sub"), None)
    return jax.shard_map(
        functools.partial(local, mesh.shape["grp"], mesh.shape["sub"]),
        mesh=mesh,
        in_specs=(rows, rows, rows, rows, P(), P()),
        out_specs=(rows, rows, rows),
        check_vma=False,
    )
```

```python
import functools

import jax
import jax.numpy as jnp
from jax import lax
from jax.experimental import pallas as pl
from jax.experimental.pallas import tpu as pltpu
from jax.sharding import PartitionSpec as P

LAYERS = 8
LANES = 128
TILE = 8
PIECES = 4
MESH = pl.DeviceIdType.MESH

beta_one = 0.9
beta_two = 0.999
step_count = 10
adam_eps = 1e-06
trust_eps = 1e-06
learn_rate = 0.05
decay_rate = 0.01


def xor(a, b, bound):
    total, bit = 0, 1
    while bit < bound:
        total = total + ((a // bit + b // bit) % 2) * bit
        bit *= 2
    return total


def flips(here, bound):
    steps, bit = [], 1
    while bit < bound:
        steps.append(bit - 2 * bit * ((here // bit) % 2))
        bit *= 2
    return [
        here + sum(step for b, step in enumerate(steps) if (k >> b) % 2) for k in range(bound)
    ]


def sub_order(subs):
    width = subs.bit_length() - 1
    codes = [i ^ (i >> 1) for i in range(subs)]
    return [sum(((c >> b) & 1) << (width - 1 - b) for b in range(width)) for c in codes]


def prepare(groups, subs, partner, ids, master_hbm, one_hbm, two_hbm, staged, row_ids,
            master, one, two, load_sem):
    devices = groups * subs
    rows_dev, width = master.shape
    block = rows_dev // devices
    many = TILE // block
    me = lax.axis_index("grp") * subs + lax.axis_index("sub")
    loads = [
        pltpu.make_async_copy(src, dst, load_sem.at[i])
        for i, (src, dst) in enumerate([(master_hbm, master), (one_hbm, one), (two_hbm, two)])
    ]
    for load in loads:
        load.start()

    def rank_of(device):
        def seek(n, found):
            return found + jnp.where(partner[n] == device, n, 0)

        return lax.fori_loop(0, devices, seek, jnp.int32(0), unroll=8)

    my_rank = rank_of(me)
    sub_iota = lax.broadcasted_iota(jnp.int32, (TILE, LANES), 0)

    def name_rows(s, carry):
        here = jnp.zeros((TILE, LANES), jnp.int32)
        for i in range(many):
            for b in range(block):
                tensor = ids[(s * many + i) * rows_dev + my_rank * block + b]
                here = jnp.where(sub_iota == i * block + b, tensor, here)
        row_ids[pl.ds(pl.multiple_of(s * TILE, TILE), TILE), :] = here
        return carry

    lax.fori_loop(0, rows_dev // TILE, name_rows, 0)
    for load in loads:
        load.wait()

    def stage(n, carry):
        peer = partner[n]
        base = pl.multiple_of((n // many) * TILE, TILE)
        part = n % many
        for a, source in enumerate((master, one, two)):
            rows = source[pl.ds(base, TILE), :]
            piece = rows[:block]
            for i in range(1, many):
                piece = jnp.where(part == i, rows[i * block : (i + 1) * block], piece)
            staged[peer, a] = piece
        return carry

    lax.fori_loop(0, devices, stage, 0)


def kernel(groups, subs, staged, row_ids, grad_hbm,
           weights, update, first_out, second_out, ratio_out,
           grad, landed, acc_w, acc_u, sums,
           load_sem, send_sem, recv_sem, sum_send, sum_recv):
    devices = groups * subs
    rows_dev, width = grad.shape
    block = rows_dev // devices
    many = TILE // block
    halves = subs // many
    columns = width // LANES
    my_grp, my_sub = lax.axis_index("grp"), lax.axis_index("sub")
    me = my_grp * subs + my_sub
    grps, sbs = flips(my_grp, groups), flips(my_sub, subs)
    order = sub_order(subs)
    peers = [g * subs + s for s in order for g in range(groups) if g or s]

    def at(k):
        return {"grp": grps[k // subs], "sub": sbs[k % subs]}

    load = pltpu.make_async_copy(grad_hbm, grad, load_sem)
    load.start()
    barrier = pltpu.get_barrier_semaphore()
    for k in reversed(peers):
        pl.semaphore_signal(barrier, inc=1, device_id=at(k), device_id_type=MESH)
    pl.semaphore_wait(barrier, devices - 1)

    def exchange(k):
        return pltpu.make_async_remote_copy(
            src_ref=staged.at[grps[k // subs] * subs + sbs[k % subs]],
            dst_ref=landed.at[k],
            send_sem=send_sem.at[k],
            recv_sem=recv_sem.at[k],
            device_id=at(k),
            device_id_type=MESH,
        )

    def exchange_sum(k):
        return pltpu.make_async_remote_copy(
            src_ref=sums.at[0],
            dst_ref=sums.at[k],
            send_sem=sum_send.at[k],
            recv_sem=sum_recv.at[k],
            device_id=at(k),
            device_id_type=MESH,
        )

    for k in peers:
        exchange(k).start()
    landed[0] = staged[me]
    load.wait()
    acc_w[...] = jnp.zeros_like(acc_w)
    acc_u[...] = jnp.zeros_like(acc_u)
    sub_iota = lax.broadcasted_iota(jnp.int32, (TILE, LANES), 0)
    lane_iota = lax.broadcasted_iota(jnp.int32, (TILE, LANES), 1)
    scale_one = 1.0 / (1.0 - beta_one**step_count)
    scale_two = 1.0 / (1.0 - beta_two**step_count)
    within = flips(me % many, many)

    def consume(j):
        base = pl.multiple_of(xor(me // many, j, devices // many) * TILE, TILE)
        slots = [j * many + within[i] for i in range(many)]
        here = row_ids[pl.ds(base, TILE), :]
        sum_w = jnp.zeros((TILE, LANES), jnp.float32)
        sum_u = jnp.zeros((TILE, LANES), jnp.float32)
        for c in range(columns):
            cut = slice(c * LANES, (c + 1) * LANES)

            def arrived(a):
                return jnp.concatenate([landed[slot, a, :, cut] for slot in slots], axis=0)

            g = grad[pl.ds(base, TILE), cut]
            w = arrived(0)
            first = beta_one * arrived(1) + (1.0 - beta_one) * g
            second = beta_two * arrived(2) + (1.0 - beta_two) * g * g
            u = (first * scale_one) / (jnp.sqrt(second * scale_two) + adam_eps) + decay_rate * w
            first_out[pl.ds(base, TILE), cut] = first
            second_out[pl.ds(base, TILE), cut] = second
            weights[pl.ds(base, TILE), cut] = w
            update[pl.ds(base, TILE), cut] = u
            sum_w += w * w
            sum_u += u * u
        for t in range(LAYERS):
            acc_w[t] += jnp.where(here == t, sum_w, 0.0)
            acc_u[t] += jnp.where(here == t, sum_u, 0.0)

    def receive(j, carry):
        for i in range(many):
            pltpu.make_async_remote_copy(
                src_ref=staged.at[0],
                dst_ref=landed.at[j * many + i],
                send_sem=send_sem.at[j * many + i],
                recv_sem=recv_sem.at[j * many + i],
                device_id=at(1),
                device_id_type=MESH,
            ).wait_recv()
        consume(j)
        return carry

    for h in sorted(range(halves), key=lambda h: max(order.index(h * many + i) for i in range(many))):
        if h == 0:
            for i in range(1, many):
                exchange(i).wait_recv()
            consume(0)
        lax.fori_loop(1 if h == 0 else 0, groups, lambda g, c, h=h: receive(g * halves + h, c), 0)

    col_w = jnp.sum(jnp.sum(acc_w[...], axis=1), axis=1, keepdims=True)
    col_u = jnp.sum(jnp.sum(acc_u[...], axis=1), axis=1, keepdims=True)
    spread = jnp.where(lane_iota == sub_iota, col_w, 0.0) + jnp.where(
        lane_iota == sub_iota + LAYERS, col_u, 0.0
    )
    sums[0] = jnp.sum(spread, axis=0, keepdims=True)
    for k in reversed(peers):
        exchange(k).wait_send()
    for k in reversed(range(1, devices)):
        exchange_sum(k).start()
    for k in range(1, devices):
        exchange_sum(k).wait_recv()
    for k in range(1, devices):
        exchange_sum(k).wait_send()
    mine = flips(me, devices)
    total = jnp.zeros((1, LANES), jnp.float32)
    for o in range(devices):
        total = total + sums[mine[o]]
    wide = jnp.broadcast_to(total, (TILE, LANES))
    weight_sq = jnp.sum(jnp.where(lane_iota == sub_iota, wide, 0.0), axis=1, keepdims=True)
    update_sq = jnp.sum(jnp.where(lane_iota == sub_iota + LAYERS, wide, 0.0), axis=1, keepdims=True)
    ratio = learn_rate * (jnp.sqrt(weight_sq) / (jnp.sqrt(update_sq) + trust_eps))
    ratio_out[...] = jnp.broadcast_to(ratio, (TILE, LANES))


def finish(ratio_ref, row_ids, weights, update, first, second,
           fresh_hbm, first_hbm, second_hbm, fresh, fresh_sem, moment_sem):
    rows_dev, width = weights.shape
    columns = width // LANES
    moments = [
        pltpu.make_async_copy(first, first_hbm, moment_sem.at[0]),
        pltpu.make_async_copy(second, second_hbm, moment_sem.at[1]),
    ]
    for move in moments:
        move.start()
    ratio = ratio_ref[...]
    span = rows_dev // PIECES
    moves = []
    for p in range(PIECES):

        def step_rows(s, carry):
            base = pl.multiple_of(p * span + s * TILE, TILE)
            here = row_ids[pl.ds(base, TILE), :]
            step = jnp.zeros((TILE, LANES), jnp.float32)
            for t in range(LAYERS):
                step = jnp.where(here == t, jnp.broadcast_to(ratio[t : t + 1], (TILE, LANES)), step)
            for c in range(columns):
                cut = slice(c * LANES, (c + 1) * LANES)
                rows = pl.ds(base, TILE)
                fresh[rows, cut] = weights[rows, cut] - step * update[rows, cut]
            return carry

        lax.fori_loop(0, span // TILE, step_rows, 0)
        rows = pl.ds(p * span, span)
        moves.append(pltpu.make_async_copy(fresh.at[rows], fresh_hbm.at[rows], fresh_sem.at[p]))
        if p:
            moves[p - 1].start()
    moves[-1].start()
    for move in moves + moments:
        move.wait()


def local(groups, subs, master, moment_one, moment_two, gradient, partner, tensor_of_row):
    rows_dev, width = master.shape
    devices = groups * subs
    block = rows_dev // devices
    whole = jax.ShapeDtypeStruct((rows_dev, width), jnp.float32)
    vmem = pl.BlockSpec(memory_space=pltpu.VMEM)
    smem = pl.BlockSpec(memory_space=pltpu.SMEM)
    hbm = pl.BlockSpec(memory_space=pltpu.HBM)
    slots = (devices, 3, block, width)
    staged, row_ids = pl.pallas_call(
        functools.partial(prepare, groups, subs),
        out_shape=(
            pltpu.VMEM(slots, jnp.float32),
            pltpu.VMEM((rows_dev, LANES), jnp.int32),
        ),
        in_specs=[smem, smem, hbm, hbm, hbm],
        out_specs=(vmem, vmem),
        scratch_shapes=[pltpu.VMEM((rows_dev, width), jnp.float32)] * 3
        + [pltpu.SemaphoreType.DMA((3,))],
        compiler_params=pltpu.CompilerParams(vmem_limit_bytes=54 * 1024 * 1024),
    )(partner, tensor_of_row, master, moment_one, moment_two)
    weights, update, first, second, ratio = pl.pallas_call(
        functools.partial(kernel, groups, subs),
        out_shape=(whole, whole, whole, whole, jax.ShapeDtypeStruct((LAYERS, LANES), jnp.float32)),
        in_specs=[vmem, vmem, hbm],
        out_specs=(vmem, vmem, vmem, vmem, vmem),
        scratch_shapes=[
            pltpu.VMEM((rows_dev, width), jnp.float32),
            pltpu.VMEM(slots, jnp.float32),
            pltpu.VMEM((LAYERS, TILE, LANES), jnp.float32),
            pltpu.VMEM((LAYERS, TILE, LANES), jnp.float32),
            pltpu.VMEM((devices, 1, LANES), jnp.float32),
            pltpu.SemaphoreType.DMA,
            pltpu.SemaphoreType.DMA((devices,)),
            pltpu.SemaphoreType.DMA((devices,)),
            pltpu.SemaphoreType.DMA((devices,)),
            pltpu.SemaphoreType.DMA((devices,)),
        ],
        compiler_params=pltpu.CompilerParams(
            collective_id=0, has_side_effects=True, vmem_limit_bytes=32 * 1024 * 1024
        ),
    )(staged, row_ids, gradient)
    return pl.pallas_call(
        finish,
        out_shape=(whole, whole, whole),
        in_specs=[vmem] * 6,
        out_specs=(hbm, hbm, hbm),
        scratch_shapes=[
            pltpu.VMEM((rows_dev, width), jnp.float32),
            pltpu.SemaphoreType.DMA((PIECES,)),
            pltpu.SemaphoreType.DMA((2,)),
        ],
        compiler_params=pltpu.CompilerParams(vmem_limit_bytes=32 * 1024 * 1024),
    )(ratio, row_ids, weights, update, first, second)


def solution(mesh):
    rows = P(("grp", "sub"), None)
    return jax.shard_map(
        functools.partial(local, mesh.shape["grp"], mesh.shape["sub"]),
        mesh=mesh,
        in_specs=(rows, rows, rows, rows, P(), P()),
        out_specs=(rows, rows, rows),
        check_vma=False,
    )
```

```python
import functools

import jax
import jax.numpy as jnp
from jax import lax
from jax.experimental import pallas as pl
from jax.experimental.pallas import tpu as pltpu
from jax.sharding import PartitionSpec as P

LAYERS = 8
LANES = 128
TILE = 8
PIECES = 4
MESH = pl.DeviceIdType.MESH

beta_one = 0.9
beta_two = 0.999
step_count = 10
adam_eps = 1e-06
trust_eps = 1e-06
learn_rate = 0.05
decay_rate = 0.01


def xor(a, b, bound):
    total, bit = 0, 1
    while bit < bound:
        total = total + ((a // bit + b // bit) % 2) * bit
        bit *= 2
    return total


def flips(here, bound):
    steps, bit = [], 1
    while bit < bound:
        steps.append(bit - 2 * bit * ((here // bit) % 2))
        bit *= 2
    return [
        here + sum(step for b, step in enumerate(steps) if (k >> b) % 2) for k in range(bound)
    ]


def sub_order(subs):
    width = subs.bit_length() - 1
    codes = [i ^ (i >> 1) for i in range(subs)]
    return [sum(((c >> b) & 1) << (width - 1 - b) for b in range(width)) for c in codes]


def prepare(groups, subs, partner, ids, master_hbm, one_hbm, two_hbm, staged, row_ids,
            master, one, two, load_sem):
    devices = groups * subs
    rows_dev, width = master.shape
    block = rows_dev // devices
    many = TILE // block
    me = lax.axis_index("grp") * subs + lax.axis_index("sub")
    loads = [
        pltpu.make_async_copy(src, dst, load_sem.at[i])
        for i, (src, dst) in enumerate([(master_hbm, master), (one_hbm, one), (two_hbm, two)])
    ]
    for load in loads:
        load.start()

    def rank_of(device):
        def seek(n, found):
            return found + jnp.where(partner[n] == device, n, 0)

        return lax.fori_loop(0, devices, seek, jnp.int32(0), unroll=8)

    my_rank = rank_of(me)
    sub_iota = lax.broadcasted_iota(jnp.int32, (TILE, LANES), 0)

    def name_rows(s):
        here = jnp.zeros((TILE, LANES), jnp.int32)
        for i in range(many):
            for b in range(block):
                tensor = ids[(s * many + i) * rows_dev + my_rank * block + b]
                here = jnp.where(sub_iota == i * block + b, tensor, here)
        row_ids[pl.ds(pl.multiple_of(s * TILE, TILE), TILE), :] = here

    for a, source in enumerate((master, one, two)):
        loads[a].wait()

        def stage(s, carry, a=a, source=source):
            rows = source[pl.ds(pl.multiple_of(s * TILE, TILE), TILE), :]
            for i in range(many):
                staged[partner[s * many + i], a] = rows[i * block : (i + 1) * block]
            if a == 0:
                name_rows(s)
            return carry

        lax.fori_loop(0, rows_dev // TILE, stage, 0)


def kernel(groups, subs, staged, row_ids, grad_hbm,
           weights, update, first_out, second_out, ratio_out,
           grad, landed, acc_w, acc_u, sums,
           load_sem, send_sem, recv_sem, sum_send, sum_recv):
    devices = groups * subs
    rows_dev, width = grad.shape
    block = rows_dev // devices
    many = TILE // block
    halves = subs // many
    columns = width // LANES
    my_grp, my_sub = lax.axis_index("grp"), lax.axis_index("sub")
    me = my_grp * subs + my_sub
    grps, sbs = flips(my_grp, groups), flips(my_sub, subs)
    order = sub_order(subs)
    peers = [g * subs + s for s in order for g in range(groups) if g or s]

    def at(k):
        return {"grp": grps[k // subs], "sub": sbs[k % subs]}

    load = pltpu.make_async_copy(grad_hbm, grad, load_sem)
    load.start()
    barrier = pltpu.get_barrier_semaphore()
    for k in reversed(peers):
        pl.semaphore_signal(barrier, inc=1, device_id=at(k), device_id_type=MESH)
    pl.semaphore_wait(barrier, devices - 1)

    def exchange(k):
        return pltpu.make_async_remote_copy(
            src_ref=staged.at[grps[k // subs] * subs + sbs[k % subs]],
            dst_ref=landed.at[k],
            send_sem=send_sem.at[k],
            recv_sem=recv_sem.at[k],
            device_id=at(k),
            device_id_type=MESH,
        )

    def exchange_sum(k):
        return pltpu.make_async_remote_copy(
            src_ref=sums.at[0],
            dst_ref=sums.at[k],
            send_sem=sum_send.at[k],
            recv_sem=sum_recv.at[k],
            device_id=at(k),
            device_id_type=MESH,
        )

    for k in peers:
        exchange(k).start()
    landed[0] = staged[me]
    load.wait()
    acc_w[...] = jnp.zeros_like(acc_w)
    acc_u[...] = jnp.zeros_like(acc_u)
    sub_iota = lax.broadcasted_iota(jnp.int32, (TILE, LANES), 0)
    lane_iota = lax.broadcasted_iota(jnp.int32, (TILE, LANES), 1)
    scale_one = 1.0 / (1.0 - beta_one**step_count)
    scale_two = 1.0 / (1.0 - beta_two**step_count)
    within = flips(me % many, many)

    def consume(j):
        base = pl.multiple_of(xor(me // many, j, devices // many) * TILE, TILE)
        slots = [j * many + within[i] for i in range(many)]
        here = row_ids[pl.ds(base, TILE), :]
        sum_w = jnp.zeros((TILE, LANES), jnp.float32)
        sum_u = jnp.zeros((TILE, LANES), jnp.float32)
        for c in range(columns):
            cut = slice(c * LANES, (c + 1) * LANES)

            def arrived(a):
                return jnp.concatenate([landed[slot, a, :, cut] for slot in slots], axis=0)

            g = grad[pl.ds(base, TILE), cut]
            w = arrived(0)
            first = beta_one * arrived(1) + (1.0 - beta_one) * g
            second = beta_two * arrived(2) + (1.0 - beta_two) * g * g
            u = (first * scale_one) / (jnp.sqrt(second * scale_two) + adam_eps) + decay_rate * w
            first_out[pl.ds(base, TILE), cut] = first
            second_out[pl.ds(base, TILE), cut] = second
            weights[pl.ds(base, TILE), cut] = w
            update[pl.ds(base, TILE), cut] = u
            sum_w += w * w
            sum_u += u * u
        for t in range(LAYERS):
            acc_w[t] += jnp.where(here == t, sum_w, 0.0)
            acc_u[t] += jnp.where(here == t, sum_u, 0.0)

    def receive(j, carry):
        for i in range(many):
            pltpu.make_async_remote_copy(
                src_ref=staged.at[0],
                dst_ref=landed.at[j * many + i],
                send_sem=send_sem.at[j * many + i],
                recv_sem=recv_sem.at[j * many + i],
                device_id=at(1),
                device_id_type=MESH,
            ).wait_recv()
        consume(j)
        return carry

    for h in sorted(range(halves), key=lambda h: max(order.index(h * many + i) for i in range(many))):
        if h == 0:
            for i in range(1, many):
                exchange(i).wait_recv()
            consume(0)
        lax.fori_loop(1 if h == 0 else 0, groups, lambda g, c, h=h: receive(g * halves + h, c), 0)

    col_w = jnp.sum(jnp.sum(acc_w[...], axis=1), axis=1, keepdims=True)
    col_u = jnp.sum(jnp.sum(acc_u[...], axis=1), axis=1, keepdims=True)
    spread = jnp.where(lane_iota == sub_iota, col_w, 0.0) + jnp.where(
        lane_iota == sub_iota + LAYERS, col_u, 0.0
    )
    sums[0] = jnp.sum(spread, axis=0, keepdims=True)
    for k in reversed(peers):
        exchange_sum(k).start()
    for k in peers:
        exchange(k).wait_send()
    for k in range(1, devices):
        exchange_sum(k).wait_recv()
    for k in range(1, devices):
        exchange_sum(k).wait_send()
    mine = flips(me, devices)
    total = jnp.zeros((1, LANES), jnp.float32)
    for o in range(devices):
        total = total + sums[mine[o]]
    wide = jnp.broadcast_to(total, (TILE, LANES))
    weight_sq = jnp.sum(jnp.where(lane_iota == sub_iota, wide, 0.0), axis=1, keepdims=True)
    update_sq = jnp.sum(jnp.where(lane_iota == sub_iota + LAYERS, wide, 0.0), axis=1, keepdims=True)
    ratio = learn_rate * (jnp.sqrt(weight_sq) / (jnp.sqrt(update_sq) + trust_eps))
    ratio_out[...] = jnp.broadcast_to(ratio, (TILE, LANES))


def finish(ratio_ref, row_ids, weights, update, first, second,
           fresh_hbm, first_hbm, second_hbm, fresh, fresh_sem, moment_sem):
    rows_dev, width = weights.shape
    columns = width // LANES
    moments = [
        pltpu.make_async_copy(first, first_hbm, moment_sem.at[0]),
        pltpu.make_async_copy(second, second_hbm, moment_sem.at[1]),
    ]
    for move in moments:
        move.start()
    ratio = ratio_ref[...]
    span = rows_dev // PIECES
    moves = []
    for p in range(PIECES):

        def step_rows(s, carry):
            base = pl.multiple_of(p * span + s * TILE, TILE)
            here = row_ids[pl.ds(base, TILE), :]
            step = jnp.zeros((TILE, LANES), jnp.float32)
            for t in range(LAYERS):
                step = jnp.where(here == t, jnp.broadcast_to(ratio[t : t + 1], (TILE, LANES)), step)
            for c in range(columns):
                cut = slice(c * LANES, (c + 1) * LANES)
                rows = pl.ds(base, TILE)
                fresh[rows, cut] = weights[rows, cut] - step * update[rows, cut]
            return carry

        lax.fori_loop(0, span // TILE, step_rows, 0)
        rows = pl.ds(p * span, span)
        moves.append(pltpu.make_async_copy(fresh.at[rows], fresh_hbm.at[rows], fresh_sem.at[p]))
        if p:
            moves[p - 1].start()
    moves[-1].start()
    for move in moves + moments:
        move.wait()


def local(groups, subs, master, moment_one, moment_two, gradient, partner, tensor_of_row):
    rows_dev, width = master.shape
    devices = groups * subs
    block = rows_dev // devices
    whole = jax.ShapeDtypeStruct((rows_dev, width), jnp.float32)
    vmem = pl.BlockSpec(memory_space=pltpu.VMEM)
    smem = pl.BlockSpec(memory_space=pltpu.SMEM)
    hbm = pl.BlockSpec(memory_space=pltpu.HBM)
    slots = (devices, 3, block, width)
    staged, row_ids = pl.pallas_call(
        functools.partial(prepare, groups, subs),
        out_shape=(
            pltpu.VMEM(slots, jnp.float32),
            pltpu.VMEM((rows_dev, LANES), jnp.int32),
        ),
        in_specs=[smem, smem, hbm, hbm, hbm],
        out_specs=(vmem, vmem),
        scratch_shapes=[pltpu.VMEM((rows_dev, width), jnp.float32)] * 3
        + [pltpu.SemaphoreType.DMA((3,))],
        compiler_params=pltpu.CompilerParams(vmem_limit_bytes=54 * 1024 * 1024),
    )(partner, tensor_of_row, master, moment_one, moment_two)
    weights, update, first, second, ratio = pl.pallas_call(
        functools.partial(kernel, groups, subs),
        out_shape=(whole, whole, whole, whole, jax.ShapeDtypeStruct((LAYERS, LANES), jnp.float32)),
        in_specs=[vmem, vmem, hbm],
        out_specs=(vmem, vmem, vmem, vmem, vmem),
        scratch_shapes=[
            pltpu.VMEM((rows_dev, width), jnp.float32),
            pltpu.VMEM(slots, jnp.float32),
            pltpu.VMEM((LAYERS, TILE, LANES), jnp.float32),
            pltpu.VMEM((LAYERS, TILE, LANES), jnp.float32),
            pltpu.VMEM((devices, 1, LANES), jnp.float32),
            pltpu.SemaphoreType.DMA,
            pltpu.SemaphoreType.DMA((devices,)),
            pltpu.SemaphoreType.DMA((devices,)),
            pltpu.SemaphoreType.DMA((devices,)),
            pltpu.SemaphoreType.DMA((devices,)),
        ],
        compiler_params=pltpu.CompilerParams(
            collective_id=0, has_side_effects=True, vmem_limit_bytes=32 * 1024 * 1024
        ),
    )(staged, row_ids, gradient)
    return pl.pallas_call(
        finish,
        out_shape=(whole, whole, whole),
        in_specs=[vmem] * 6,
        out_specs=(hbm, hbm, hbm),
        scratch_shapes=[
            pltpu.VMEM((rows_dev, width), jnp.float32),
            pltpu.SemaphoreType.DMA((PIECES,)),
            pltpu.SemaphoreType.DMA((2,)),
        ],
        compiler_params=pltpu.CompilerParams(vmem_limit_bytes=32 * 1024 * 1024),
    )(ratio, row_ids, weights, update, first, second)


def solution(mesh):
    rows = P(("grp", "sub"), None)
    return jax.shard_map(
        functools.partial(local, mesh.shape["grp"], mesh.shape["sub"]),
        mesh=mesh,
        in_specs=(rows, rows, rows, rows, P(), P()),
        out_specs=(rows, rows, rows),
        check_vma=False,
    )
```
